32 devices in a mesh: rows: 8 (over y, x, core), cols: 4 (over z).
Axes of the slice: x: 2, y: 2, z: 4, core: 2. Of those that a mesh axis runs over, the one named last changes fastest.
Arguments:
- token_ids: int32 [16, 2048], P('rows', 'cols'), may hold values from 0 to 131071, as said below
- lengths: int32 [16], P('rows'), may hold values from 1 to 2048
- table: bfloat16 [131072, 512], P('rows', 'cols'), may hold values from -6 to 6
- attn_gain: float32 [512], replicated, may hold values from 0.1 to 1.9
- w_qkv: bfloat16 [512, 1536], replicated, may hold values from -2 to 2
- w_out: bfloat16 [512, 512], replicated, may hold values from -0.25 to 0.25
- mlp_gain: float32 [512], replicated, may hold values from 0.1 to 1.9
- w_in: bfloat16 [512, 4096], replicated, may hold values from -0.25 to 0.25
- w_down: bfloat16 [2048, 512], replicated, may hold values from -0.125 to 0.125
Outputs:
- layer_out: bfloat16 [16, 2048, 512], P('rows', 'cols')
The draws below stay inside these ranges and needn't reach their ends.
Inputs may be any that keep to these rules, and one draw needn't show every extreme that they name: `token_ids`: ids lie in 0 to 131071. In each aligned block of 2 histories (4096 positions) at most 1365 ids fall in any one block of 16384 consecutive table rows, and in every such block of histories some block of table rows receives exactly 1365.
All inputs are finite; a program needn't handle non-finite values.
Results may differ from the reference program's by a relative error of at most 0.012.
Values may be sent and summed in bfloat16 or wider, within the bound.
A program may use at most 192 MiB of HBM per device.

```python
import jax
import jax.numpy as jnp
from jax import lax

D = 512
HEADS = 8
FF = 2048
VOC_DEV = 16384
BD = 2
L = 2048
B = 16
VOCAB = 131072
CAP = 1365


def one_block(key):
    key_hot, key_order, key_shuffle, key_offset = jax.random.split(key, 4)
    block_count = B // BD
    token_count = BD * L
    hot_block = jax.random.randint(key_hot, (), 0, block_count)
    slot_ids = jnp.arange(block_count * CAP, dtype=jnp.int32)
    slot_block = slot_ids // CAP
    order_rank = jax.random.permutation(key_order, block_count * CAP).astype(jnp.int32)
    priority = jnp.where(slot_block == hot_block, 0, 1) * (block_count * CAP) + order_rank
    chosen_order = jnp.argsort(priority)
    chosen_block = slot_block[chosen_order[:token_count]]
    chosen_block = jax.random.permutation(key_shuffle, chosen_block)
    offsets = jax.random.randint(key_offset, (token_count,), 0, VOC_DEV)
    return (chosen_block * VOC_DEV + offsets).astype(jnp.int32).reshape(BD, L)


def draw_token_ids(key, part):
    keys = jax.random.split(jax.random.fold_in(key, 11), B // BD)
    return jax.vmap(one_block)(keys).reshape(B, L)


def draw_w_qkv(key, part):
    key_base = jax.random.fold_in(jax.random.fold_in(key, 23), 0)
    base = jnp.clip(jax.random.normal(key_base, (D, 3 * D), jnp.float32), -5.0, 5.0) / jnp.sqrt(1.0 * D)
    return jnp.clip(base, -2.0, 2.0).astype(jnp.bfloat16)


def touch_ends(drawn, stream_key, low, top_value):
    longest = drawn.shape.index(max(drawn.shape))
    spots = []
    for shift in (0, 1):
        where = [jax.random.randint(jax.random.fold_in(stream_key, axis), (), 0, length) for axis, length in enumerate(drawn.shape)]
        where[longest] = (where[longest] + shift) % drawn.shape[longest]
        spots.append(tuple(where))
    return drawn.at[spots[0]].set(low).at[spots[1]].set(top_value)


def block_scale(stream_key, extent, shards, low, largest):
    loudness = 1.0
    for axis_at, parts in shards:
        draws = jax.random.uniform(jax.random.fold_in(jax.random.fold_in(stream_key, 6), axis_at), (parts,), jnp.float32, low / len(shards), largest / len(shards))
        loudness = loudness * jnp.repeat(jnp.exp(draws), extent[axis_at] // parts).reshape((-1,) + (1,) * (len(extent) - 1 - axis_at))
    return loudness


def centred(key, shape, scale, most, cuts=(), kind=jnp.bfloat16):
    factor_of = block_scale(key, shape, cuts, -0.22, 0.18) if cuts else 1.0
    entries = jax.random.normal(key, shape, jnp.float32) * scale * factor_of
    return jnp.minimum(jnp.maximum(entries, -most), most).astype(kind)


def setup_inputs(seed: int = 0) -> dict:
    streams_of = jax.random.split(jax.random.key(seed), 10)
    return {
        "token_ids": draw_token_ids(jax.random.fold_in(streams_of[9], 71), 0),
        "lengths": touch_ends(jax.random.randint(streams_of[1], (B,), 1, L + 1), jax.random.fold_in(streams_of[1], 1), 1, L).astype(jnp.int32),
        "table": centred(streams_of[2], (VOCAB, D), 1.0, 6.0, ((0, 8), (1, 4))),
        "attn_gain": jnp.clip(1.0 + 0.18 * jax.random.normal(streams_of[3], (D,), jnp.float32), 0.1, 1.9),
        "w_qkv": draw_w_qkv(jax.random.fold_in(streams_of[9], 71), 0),
        "w_out": centred(streams_of[5], (D, D), D ** -0.5, 0.25),
        "mlp_gain": jnp.clip(1.0 + 0.18 * jax.random.normal(streams_of[6], (D,), jnp.float32), 0.1, 1.9),
        "w_in": centred(streams_of[7], (D, 2 * FF), D ** -0.5, 0.25),
        "w_down": centred(streams_of[8], (FF, D), FF ** -0.5, 0.125),
    }


def rms_norm(values_f32, gain):
    mean_sq = lax.optimization_barrier(jnp.mean(values_f32 * values_f32, axis=-1, keepdims=True))
    return values_f32 * lax.rsqrt(mean_sq + 1e-06) * gain

def layer(sequence, length, attn_gain, w_qkv, w_out, mlp_gain, w_in, w_down):
    residual = sequence.astype(jnp.float32)
    normed = rms_norm(residual, attn_gain).astype(jnp.bfloat16)
    projected = jnp.dot(normed, w_qkv, preferred_element_type=jnp.float32).astype(jnp.bfloat16)
    head_dim = D // HEADS
    queries = projected[:, :D].reshape(L, HEADS, head_dim).astype(jnp.float32)
    keys = projected[:, D:2 * D].reshape(L, HEADS, head_dim).astype(jnp.float32)
    values = projected[:, 2 * D:].reshape(L, HEADS, head_dim).astype(jnp.float32)
    scores = jnp.einsum('qhd,khd->hqk', queries, keys) * 0.125
    position = jnp.arange(L, dtype=jnp.int32)
    valid = (position[None, :] <= position[:, None]) & (position[None, :] < length)
    valid = valid[None, :, :]
    scores = jnp.where(valid, scores, -1e+30)
    row_max = lax.optimization_barrier(jnp.max(scores, axis=-1, keepdims=True))
    probs = jnp.where(valid, jnp.exp(scores - row_max), 0.0)
    total = lax.optimization_barrier(jnp.sum(probs, axis=-1))
    weights = probs.astype(jnp.bfloat16).astype(jnp.float32)
    summed = jnp.einsum('hqk,khd->hqd', weights, values) / total[..., None]
    attended = jnp.transpose(summed, (1, 0, 2)).reshape(L, D).astype(jnp.bfloat16)
    hidden = (residual + jnp.dot(attended, w_out, preferred_element_type=jnp.float32)).astype(jnp.bfloat16)
    hidden_f32 = hidden.astype(jnp.float32)
    normed_two = rms_norm(hidden_f32, mlp_gain).astype(jnp.bfloat16)
    gate_up = jnp.dot(normed_two, w_in, preferred_element_type=jnp.float32)
    act = (jax.nn.silu(gate_up[:, :FF]) * gate_up[:, FF:]).astype(jnp.bfloat16)
    return (hidden_f32 + jnp.dot(act, w_down, preferred_element_type=jnp.float32)).astype(jnp.bfloat16)

def reference(token_ids, lengths, table, attn_gain, w_qkv, w_out, mlp_gain, w_in, w_down):
    embedded = jnp.take(table, token_ids, axis=0)

    def one_history(pair):
        sequence, length = pair
        return layer(sequence, length, attn_gain, w_qkv, w_out, mlp_gain, w_in, w_down)
    return lax.map(one_history, (embedded, lengths))
```

```python
import functools

import jax
import jax.numpy as jnp
from jax import lax
from jax.experimental import pallas as pl
from jax.experimental.pallas import tpu as pltpu
from jax.sharding import PartitionSpec as P

HEADS = 8
LANES = 128
NEG = -1e30
SCORE_SCALE = 0.125 * 1.4426950408889634
MESH = pl.DeviceIdType.MESH
BF = jnp.bfloat16
F32 = jnp.float32


def rms_norm(values_f32, gain):
    mean_sq = jnp.mean(values_f32 * values_f32, axis=-1, keepdims=True)
    return values_f32 * lax.rsqrt(mean_sq + 1e-06) * gain


def layer_kernel(
    cols, lens_ref, e_ref, gain1, gain2, wq_h, wk_h, wv_h, wo_h, wi_h, wd_h, out_ref,
    ebuf, wq, wk, wv, wo, wi, wd, qm, k_s, v_s, m_s, l_s, acc,
    send_sem, recv_sem, own_sem, w_sem,
):
    me = lax.axis_index("cols")
    batch, full, width = e_ref.shape
    quarter = full // cols
    head_dim = LANES // 2

    def chunk(j):
        return pl.ds(pl.multiple_of(j * quarter, quarter), quarter)

    def slice_copy(b, source, target, j):
        return pltpu.make_async_remote_copy(
            src_ref=e_ref.at[b, chunk(j)],
            dst_ref=ebuf.at[source, b, chunk(j)],
            send_sem=send_sem.at[b, target, j],
            recv_sem=recv_sem.at[b, source, j],
            device_id={"cols": target},
            device_id_type=MESH,
        )

    barrier = pltpu.get_barrier_semaphore()
    for off in range(1, cols):
        pl.semaphore_signal(
            barrier, inc=1, device_id={"cols": lax.rem(me + off, cols)}, device_id_type=MESH
        )
    pl.semaphore_wait(barrier, cols - 1)

    def for_sends(act):
        def step(i, carry):
            b, t = i // cols, lax.rem(i, cols)
            for d in reversed(range(cols)):
                j = jnp.where(t == 0, d, t - 1)

                @pl.when((me != d) & (t <= d))
                def _():
                    act(slice_copy(b, me, d, j))

            return carry

        lax.fori_loop(0, batch * cols, step, 0)

    for_sends(lambda copy: copy.start())
    own = pltpu.make_async_copy(e_ref, ebuf.at[me], own_sem)
    own.start()
    loads = [
        pltpu.make_async_copy(src, dst, w_sem.at[i])
        for i, (src, dst) in enumerate(
            ((wq_h, wq), (wk_h, wk), (wv_h, wv), (wo_h, wo), (wi_h, wi), (wd_h, wd))
        )
    ]
    for load in loads:
        load.start()
    own.wait()
    for load in loads:
        load.wait()

    dims_nt = (((1,), (1,)), ((), ()))

    def embedded(b, j):
        parts = [ebuf[s, b, chunk(j), :] for s in range(cols)]
        return jnp.concatenate(parts, axis=1).astype(F32)

    def history(b, carry):
        length = lens_ref[b]
        query_pos = me * quarter + lax.broadcasted_iota(jnp.int32, (1, quarter), 1)
        limit = jnp.minimum(query_pos + 1, length)

        def unit(t, carry):
            j = jnp.where(t == 0, me, t - 1)
            for s in range(cols):

                @pl.when(me != s)
                def _():
                    slice_copy(b, s, s, j).wait_recv()

            normed = rms_norm(embedded(b, j), gain1[...]).astype(BF)
            k_s[...] = jnp.dot(normed, wk[...], preferred_element_type=F32).astype(BF)
            v_s[...] = lax.dot_general(
                wv[...], normed, dims_nt, preferred_element_type=F32
            ).astype(BF)

            @pl.when(t == 0)
            def _():
                q_t = lax.dot_general(
                    wq[...], normed, dims_nt, preferred_element_type=F32
                ).astype(BF)
                zero = jnp.zeros((head_dim, quarter), BF)
                for h in range(HEADS):
                    mine = q_t[h * head_dim : (h + 1) * head_dim]
                    pair = (mine, zero) if h % 2 == 0 else (zero, mine)
                    qm[h] = jnp.concatenate(pair, axis=0)
                m_s[...] = jnp.full_like(m_s, NEG)
                l_s[...] = jnp.zeros_like(l_s)
                acc[...] = jnp.zeros_like(acc)

            key_pos = lax.broadcasted_iota(jnp.int32, (quarter, quarter), 0)
            keep = key_pos < limit - j * quarter

            def pair(p, carry):
                k_pair = k_s[:, pl.ds(pl.multiple_of(p * LANES, LANES), LANES)]
                for side in range(2):
                    h = 2 * p + side
                    s = jnp.dot(k_pair, qm[h], preferred_element_type=F32) * SCORE_SCALE
                    s = jnp.where(keep, s, NEG)
                    m_old = m_s[h]
                    m_new = jnp.maximum(m_old, jnp.max(s, axis=0, keepdims=True))
                    probs = jnp.exp2(s - m_new)
                    alpha = jnp.exp2(m_old - m_new)
                    m_s[h] = m_new
                    l_s[h] = l_s[h] * alpha + jnp.sum(probs, axis=0, keepdims=True)
                    v_t = v_s[pl.ds(pl.multiple_of(h * head_dim, head_dim), head_dim), :]
                    acc[h] = acc[h] * alpha + jnp.dot(
                        v_t, probs.astype(BF), preferred_element_type=F32
                    )
                return carry

            lax.fori_loop(0, HEADS // 2, pair, 0)
            return carry

        lax.fori_loop(0, me + 1, unit, 0)

        att_t = (acc[...] / l_s[...]).reshape(HEADS * head_dim, quarter)
        attended = att_t.T.astype(BF)
        hidden = (
            embedded(b, me) + jnp.dot(attended, wo[...], preferred_element_type=F32)
        ).astype(BF)
        hidden = hidden.astype(F32)
        normed_two = rms_norm(hidden, gain2[...]).astype(BF)
        ff = wd.shape[0]
        tile = 512
        total = hidden
        for f in range(0, ff, tile):
            gate = jnp.dot(normed_two, wi[:, f : f + tile], preferred_element_type=F32)
            up = jnp.dot(normed_two, wi[:, ff + f : ff + f + tile], preferred_element_type=F32)
            act = (gate / (1.0 + jnp.exp(-gate)) * up).astype(BF)
            total = total + jnp.dot(act, wd[f : f + tile, :], preferred_element_type=F32)
        out_ref[b] = total.astype(BF)
        return carry

    lax.fori_loop(0, batch, history, 0)
    for_sends(lambda copy: copy.wait_send())


def layer_call(cols, lengths, emb, gain1, gain2, w_qkv, w_out, w_in, w_down):
    batch, full, width = emb.shape
    quarter = full // cols
    d = width * cols
    wq_t = w_qkv[:, :d].T
    wk = w_qkv[:, d : 2 * d]
    wv_t = w_qkv[:, 2 * d :].T
    any_spec = pl.BlockSpec(memory_space=pl.ANY)
    vmem = pl.BlockSpec(memory_space=pltpu.VMEM)
    smem = pl.BlockSpec(memory_space=pltpu.SMEM)
    weights = (wq_t, wk, wv_t, w_out, w_in, w_down)
    head_dim = d // HEADS
    return pl.pallas_call(
        functools.partial(layer_kernel, cols),
        out_shape=jax.ShapeDtypeStruct((batch, quarter, d), BF),
        in_specs=[smem, any_spec, vmem, vmem] + [any_spec] * 6,
        out_specs=vmem,
        scratch_shapes=[pltpu.VMEM((cols, batch, full, width), BF)]
        + [pltpu.VMEM(w.shape, BF) for w in weights]
        + [
            pltpu.VMEM((HEADS, 2 * head_dim, quarter), BF),
            pltpu.VMEM((quarter, d), BF),
            pltpu.VMEM((d, quarter), BF),
            pltpu.VMEM((HEADS, 1, quarter), F32),
            pltpu.VMEM((HEADS, 1, quarter), F32),
            pltpu.VMEM((HEADS, head_dim, quarter), F32),
            pltpu.SemaphoreType.DMA((batch, cols, cols)),
            pltpu.SemaphoreType.DMA((batch, cols, cols)),
            pltpu.SemaphoreType.DMA,
            pltpu.SemaphoreType.DMA((6,)),
        ],
        compiler_params=pltpu.CompilerParams(
            collective_id=0, has_side_effects=True, vmem_limit_bytes=60 * 1024 * 1024
        ),
    )(lengths, emb, gain1.reshape(1, d), gain2.reshape(1, d), *weights)


def local(token_ids, lengths, table, attn_gain, w_qkv, w_out, mlp_gain, w_in, w_down):
    batch_dev, quarter = token_ids.shape
    col_count = lax.axis_size("cols")
    row_count = lax.axis_size("rows")
    full_len = quarter * col_count
    block_rows, col_width = table.shape
    own_ids = lax.all_gather(token_ids, "cols", axis=1, tiled=True)
    flat_ids = own_ids.reshape(-1)
    token_count = flat_ids.shape[0]
    capacity = -(-(8 * token_count // (3 * row_count)) // 16) * 16
    owner_block = flat_ids // block_rows
    offset = flat_ids - owner_block * block_rows
    onehot = (owner_block[:, None] == jnp.arange(row_count, dtype=jnp.int32)[None, :]).astype(
        jnp.int32
    )
    slot_rank = jnp.sum((jnp.cumsum(onehot, axis=0) - 1) * onehot, axis=1)
    slot_index = owner_block * capacity + slot_rank
    groups = -(-capacity // LANES)
    group_id = owner_block * groups + slot_rank // LANES
    left = (group_id[:, None] == jnp.arange(row_count * groups, dtype=jnp.int32)[None, :]).astype(BF)
    lane = slot_rank % LANES
    hit = lane[:, None] == jnp.arange(LANES, dtype=jnp.int32)[None, :]
    high = jnp.where(hit, (offset // LANES)[:, None], 0).astype(BF)
    low = jnp.where(hit, (offset % LANES)[:, None], 0).astype(BF)
    high = lax.dot_general(left, high, (((0,), (0,)), ((), ())), preferred_element_type=F32)
    low = lax.dot_general(left, low, (((0,), (0,)), ((), ())), preferred_element_type=F32)
    requests = (high * LANES + low).astype(jnp.int32)
    requests = requests.reshape(row_count, groups * LANES)[:, :capacity]
    asked = lax.all_to_all(requests, "rows", split_axis=0, concat_axis=0, tiled=True)
    looked = table.at[asked.reshape(-1)].get(mode="promise_in_bounds")
    returned = lax.all_to_all(looked, "rows", split_axis=0, concat_axis=0, tiled=True)
    emb = returned.at[slot_index].get(mode="promise_in_bounds")
    emb = emb.reshape(batch_dev, full_len, col_width)
    return layer_call(
        col_count, lengths, emb, attn_gain, mlp_gain, w_qkv, w_out, w_in, w_down
    )


def solution(mesh):
    in_specs = (P("rows", "cols"), P("rows"), P("rows", "cols"), P(), P(), P(), P(), P(), P())
    out_specs = P("rows", "cols", None)
    return jax.shard_map(local, mesh=mesh, in_specs=in_specs, out_specs=out_specs, check_vma=False)
```

```python
import functools

import jax
import jax.numpy as jnp
from jax import lax
from jax.experimental import pallas as pl
from jax.experimental.pallas import tpu as pltpu
from jax.sharding import PartitionSpec as P

HEADS = 8
LANES = 128
NEG = -1e30
SCORE_SCALE = 0.125 * 1.4426950408889634
MESH = pl.DeviceIdType.MESH
BF = jnp.bfloat16
F32 = jnp.float32


def rms_norm(values_f32, gain):
    mean_sq = jnp.mean(values_f32 * values_f32, axis=-1, keepdims=True)
    return values_f32 * lax.rsqrt(mean_sq + 1e-06) * gain


def layer_kernel(
    cols, lens_ref, e_ref, gain1, gain2, wq_h, wk_h, wv_h, wo_h, wi_h, wd_h, out_ref,
    ebuf, wq, wk, wv, wo, wi, wd, qm, k_s, v_s, m_s, l_s, acc,
    send_sem, recv_sem, relay_sem, own_sem, w_sem,
):
    me = lax.axis_index("cols")
    batch, full, width = e_ref.shape
    quarter = full // cols
    head_dim = LANES // 2

    def chunk(j):
        return pl.ds(pl.multiple_of(j * quarter, quarter), quarter)

    def slice_copy(b, source, target, j):
        return pltpu.make_async_remote_copy(
            src_ref=e_ref.at[b, chunk(j)],
            dst_ref=ebuf.at[source, b, chunk(j)],
            send_sem=send_sem.at[b, target, j],
            recv_sem=recv_sem.at[b, source, j],
            device_id={"cols": target},
            device_id_type=MESH,
        )

    def relay_copy(b, source, j):
        return pltpu.make_async_remote_copy(
            src_ref=ebuf.at[source, b, chunk(j)],
            dst_ref=ebuf.at[source, b, chunk(j)],
            send_sem=relay_sem.at[b, source, j],
            recv_sem=recv_sem.at[b, source, j],
            device_id={"cols": lax.rem(me + 1, cols)},
            device_id_type=MESH,
        )

    def relays(source):
        return (me + 1 < cols) & (me + 1 - source >= 3)

    barrier = pltpu.get_barrier_semaphore()
    for off in range(1, cols):
        pl.semaphore_signal(
            barrier, inc=1, device_id={"cols": lax.rem(me + off, cols)}, device_id_type=MESH
        )
    pl.semaphore_wait(barrier, cols - 1)

    def for_sends(act):
        def step(i, carry):
            b, t = i // cols, lax.rem(i, cols)
            for d in reversed(range(cols)):
                j = jnp.where(t == 0, d, t - 1)

                @pl.when((me != d) & (t <= d) & ((d - me < 3) | (t == 0)))
                def _():
                    act(slice_copy(b, me, d, j))

            return carry

        lax.fori_loop(0, batch * cols, step, 0)

    for_sends(lambda copy: copy.start())
    own = pltpu.make_async_copy(e_ref, ebuf.at[me], own_sem)
    own.start()
    loads = [
        pltpu.make_async_copy(src, dst, w_sem.at[i])
        for i, (src, dst) in enumerate(
            ((wq_h, wq), (wk_h, wk), (wv_h, wv), (wo_h, wo), (wi_h, wi), (wd_h, wd))
        )
    ]
    for load in loads:
        load.start()
    own.wait()
    for load in loads[:3]:
        load.wait()

    dims_nt = (((1,), (1,)), ((), ()))

    def embedded(b, j):
        parts = [ebuf[s, b, chunk(j), :] for s in range(cols)]
        return jnp.concatenate(parts, axis=1).astype(F32)

    def history(b, carry):
        length = lens_ref[b]
        query_pos = me * quarter + lax.broadcasted_iota(jnp.int32, (1, quarter), 1)
        limit = jnp.minimum(query_pos + 1, length)

        def unit(t, carry):
            j = jnp.where(t == 0, me, t - 1)
            for s in range(cols):

                @pl.when(me != s)
                def _():
                    slice_copy(b, s, s, j).wait_recv()

            for s in range(cols - 3):

                @pl.when(relays(s))
                def _():
                    relay_copy(b, s, j).start()

            normed = rms_norm(embedded(b, j), gain1[...]).astype(BF)
            k_s[...] = jnp.dot(normed, wk[...], preferred_element_type=F32).astype(BF)
            v_s[...] = lax.dot_general(
                wv[...], normed, dims_nt, preferred_element_type=F32
            ).astype(BF)

            @pl.when(t == 0)
            def _():
                q_t = lax.dot_general(
                    wq[...], normed, dims_nt, preferred_element_type=F32
                ).astype(BF)
                zero = jnp.zeros((head_dim, quarter), BF)
                for h in range(HEADS):
                    mine = q_t[h * head_dim : (h + 1) * head_dim]
                    pair = (mine, zero) if h % 2 == 0 else (zero, mine)
                    qm[h] = jnp.concatenate(pair, axis=0)
                m_s[...] = jnp.full_like(m_s, NEG)
                l_s[...] = jnp.zeros_like(l_s)
                acc[...] = jnp.zeros_like(acc)

            key_pos = lax.broadcasted_iota(jnp.int32, (quarter, quarter), 0)
            keep = key_pos < limit - j * quarter

            def pair(p, carry):
                k_pair = k_s[:, pl.ds(pl.multiple_of(p * LANES, LANES), LANES)]
                for side in range(2):
                    h = 2 * p + side
                    s = jnp.dot(k_pair, qm[h], preferred_element_type=F32) * SCORE_SCALE
                    s = jnp.where(keep, s, NEG)
                    m_old = m_s[h]
                    m_new = jnp.maximum(m_old, jnp.max(s, axis=0, keepdims=True))
                    probs = jnp.exp2(s - m_new)
                    alpha = jnp.exp2(m_old - m_new)
                    m_s[h] = m_new
                    l_s[h] = l_s[h] * alpha + jnp.sum(probs, axis=0, keepdims=True)
                    v_t = v_s[pl.ds(pl.multiple_of(h * head_dim, head_dim), head_dim), :]
                    acc[h] = acc[h] * alpha + jnp.dot(
                        v_t, probs.astype(BF), preferred_element_type=F32
                    )
                return carry

            lax.fori_loop(0, HEADS // 2, pair, 0)
            return carry

        lax.fori_loop(0, me + 1, unit, 0)

        @pl.when(b == 0)
        def _():
            for load in loads[3:]:
                load.wait()

        att_t = (acc[...] / l_s[...]).reshape(HEADS * head_dim, quarter)
        attended = att_t.T.astype(BF)
        hidden = (
            embedded(b, me) + jnp.dot(attended, wo[...], preferred_element_type=F32)
        ).astype(BF)
        hidden = hidden.astype(F32)
        normed_two = rms_norm(hidden, gain2[...]).astype(BF)
        ff = wd.shape[0]
        tile = 512
        total = hidden
        for f in range(0, ff, tile):
            gate = jnp.dot(normed_two, wi[:, f : f + tile], preferred_element_type=F32)
            up = jnp.dot(normed_two, wi[:, ff + f : ff + f + tile], preferred_element_type=F32)
            act = (gate / (1.0 + jnp.exp(-gate)) * up).astype(BF)
            total = total + jnp.dot(act, wd[f : f + tile, :], preferred_element_type=F32)
        out_ref[b] = total.astype(BF)
        return carry

    lax.fori_loop(0, batch, history, 0)
    for_sends(lambda copy: copy.wait_send())

    def relay_ends(i, carry):
        for s in range(cols - 3):

            @pl.when(relays(s) & (lax.rem(i, cols) <= me))
            def _():
                relay_copy(i // cols, s, lax.rem(i, cols)).wait_send()

        return carry

    lax.fori_loop(0, batch * cols, relay_ends, 0)


def layer_call(cols, lengths, emb, gain1, gain2, w_qkv, w_out, w_in, w_down):
    batch, full, width = emb.shape
    quarter = full // cols
    d = width * cols
    wq_t = w_qkv[:, :d].T
    wk = w_qkv[:, d : 2 * d]
    wv_t = w_qkv[:, 2 * d :].T
    any_spec = pl.BlockSpec(memory_space=pl.ANY)
    vmem = pl.BlockSpec(memory_space=pltpu.VMEM)
    smem = pl.BlockSpec(memory_space=pltpu.SMEM)
    weights = (wq_t, wk, wv_t, w_out, w_in, w_down)
    head_dim = d // HEADS
    return pl.pallas_call(
        functools.partial(layer_kernel, cols),
        out_shape=jax.ShapeDtypeStruct((batch, quarter, d), BF),
        in_specs=[smem, any_spec, vmem, vmem] + [any_spec] * 6,
        out_specs=vmem,
        scratch_shapes=[pltpu.VMEM((cols, batch, full, width), BF)]
        + [pltpu.VMEM(w.shape, BF) for w in weights]
        + [
            pltpu.VMEM((HEADS, 2 * head_dim, quarter), BF),
            pltpu.VMEM((quarter, d), BF),
            pltpu.VMEM((d, quarter), BF),
            pltpu.VMEM((HEADS, 1, quarter), F32),
            pltpu.VMEM((HEADS, 1, quarter), F32),
            pltpu.VMEM((HEADS, head_dim, quarter), F32),
            pltpu.SemaphoreType.DMA((batch, cols, cols)),
            pltpu.SemaphoreType.DMA((batch, cols, cols)),
            pltpu.SemaphoreType.DMA((batch, cols, cols)),
            pltpu.SemaphoreType.DMA,
            pltpu.SemaphoreType.DMA((6,)),
        ],
        compiler_params=pltpu.CompilerParams(
            collective_id=0, has_side_effects=True, vmem_limit_bytes=60 * 1024 * 1024
        ),
    )(lengths, emb, gain1.reshape(1, d), gain2.reshape(1, d), *weights)


def local(token_ids, lengths, table, attn_gain, w_qkv, w_out, mlp_gain, w_in, w_down):
    batch_dev, quarter = token_ids.shape
    col_count = lax.axis_size("cols")
    row_count = lax.axis_size("rows")
    full_len = quarter * col_count
    block_rows, col_width = table.shape
    own_ids = lax.all_gather(token_ids, "cols", axis=1, tiled=True)
    flat_ids = own_ids.reshape(-1)
    token_count = flat_ids.shape[0]
    capacity = -(-(8 * token_count // (3 * row_count)) // 16) * 16
    owner_block = flat_ids // block_rows
    offset = flat_ids - owner_block * block_rows
    onehot = (owner_block[:, None] == jnp.arange(row_count, dtype=jnp.int32)[None, :]).astype(
        jnp.int32
    )
    slot_rank = jnp.sum((jnp.cumsum(onehot, axis=0) - 1) * onehot, axis=1)
    slot_index = owner_block * capacity + slot_rank
    groups = -(-capacity // LANES)
    group_id = owner_block * groups + slot_rank // LANES
    left = (group_id[:, None] == jnp.arange(row_count * groups, dtype=jnp.int32)[None, :]).astype(BF)
    lane = slot_rank % LANES
    hit = lane[:, None] == jnp.arange(LANES, dtype=jnp.int32)[None, :]
    high = jnp.where(hit, (offset // LANES)[:, None], 0).astype(BF)
    low = jnp.where(hit, (offset % LANES)[:, None], 0).astype(BF)
    high = lax.dot_general(left, high, (((0,), (0,)), ((), ())), preferred_element_type=F32)
    low = lax.dot_general(left, low, (((0,), (0,)), ((), ())), preferred_element_type=F32)
    requests = (high * LANES + low).astype(jnp.int32)
    requests = requests.reshape(row_count, groups * LANES)[:, :capacity]
    asked = lax.all_to_all(requests, "rows", split_axis=0, concat_axis=0, tiled=True)
    looked = table.at[asked.reshape(-1)].get(mode="promise_in_bounds")
    returned = lax.all_to_all(looked, "rows", split_axis=0, concat_axis=0, tiled=True)
    emb = returned.at[slot_index].get(mode="promise_in_bounds")
    emb = emb.reshape(batch_dev, full_len, col_width)
    return layer_call(
        col_count, lengths, emb, attn_gain, mlp_gain, w_qkv, w_out, w_in, w_down
    )


def solution(mesh):
    in_specs = (P("rows", "cols"), P("rows"), P("rows", "cols"), P(), P(), P(), P(), P(), P())
    out_specs = P("rows", "cols", None)
    return jax.shard_map(local, mesh=mesh, in_specs=in_specs, out_specs=out_specs, check_vma=False)
```
